32 devices in a mesh: grp: 8 (over y, x, core), fsdp: 4 (over z).
Axes of the slice: x: 2, y: 2, z: 4, core: 2. Of those that a mesh axis runs over, the one named last changes fastest.
Arguments:
- layer_inputs: bfloat16 [8, 2048, 2048], P('grp', 'fsdp'), may hold values from -6 to 6
- key_cotangent: bfloat16 [8, 2048, 768], P('grp', 'fsdp'), may hold values from -0.099609375 to 0.099609375
- key_weights: bfloat16 [2048, 768], P('fsdp'), may hold values from -0.125 to 0.125
- outer_momentum: float32 [2048, 768], P('fsdp'), may hold values from -0.02 to 0.02
- state_codes: int32 [8, 2048, 768], P('grp', 'fsdp'), may hold values from 0 to 255
- first_row_max: float32 [8, 2048], P('grp', 'fsdp'), may hold values from 0.1 to 2
- first_col_max: float32 [8, 768], P('grp'), may hold values from 0.1 to 2
- second_row_max: float32 [8, 2048], P('grp', 'fsdp'), may hold values from 0.1 to 4
- second_col_max: float32 [8, 768], P('grp'), may hold values from 0.1 to 4
Outputs:
- new_weights: float32 [2048, 768], P('fsdp')
- new_momentum: float32 [2048, 768], P('fsdp')
- first_state: bfloat16 [8, 2048, 768], P('grp', 'fsdp')
- second_state: bfloat16 [8, 2048, 768], P('grp', 'fsdp')
- new_first_row_max: float32 [8, 2048], P('grp', 'fsdp')
- new_first_col_max: float32 [8, 768], P('grp')
- new_second_row_max: float32 [8, 2048], P('grp', 'fsdp')
- new_second_col_max: float32 [8, 768], P('grp')
- next_keys: bfloat16 [8, 2048, 768], P('grp', 'fsdp')
The draws below stay inside these ranges and needn't reach their ends.
All inputs are finite; a program needn't handle non-finite values. Where the reference program divides by a largest or mean magnitude, that divisor is 1e-20 or more.
Results may differ from the reference program's by a relative error of at most 0.018.
Values may be sent and summed in bfloat16 or wider, within the bound.
A program may use at most 64 MiB of HBM per device.

```python
import math
import jax
import jax.numpy as jnp
from jax import lax

ROWS = 2048
COLS = 768
TOK_DEV = 512
GROUPS = 8
TOK_GRP = 2048
N_GRP = 8
N_FSDP = 4


def set_ends(result, own_key, low, top_value):
    place = [jax.random.randint(jax.random.fold_in(own_key, axis), (), 0, length) for axis, length in enumerate(result.shape)]
    main_axis = result.shape.index(max(result.shape))
    beside = place[:main_axis] + [(place[main_axis] + 1) % result.shape[main_axis]] + place[main_axis + 1:]
    return result.at[tuple(place)].set(low).at[tuple(beside)].set(top_value)


def shard_levels(own_key, shape, shards, smallest, high):
    level = 1.0
    for position, shards_of in shards:
        steps = jax.random.uniform(jax.random.fold_in(jax.random.fold_in(own_key, 6), position), (shards_of,), jnp.float32, smallest / len(shards), high / len(shards))
        level = level * jnp.repeat(jnp.exp(steps), shape[position] // shards_of).reshape((-1,) + (1,) * (len(shape) - 1 - position))
    return level


def bell_draw(stream_key, shape, width, bound, cuts=(), dtype=jnp.bfloat16):
    entries = jax.random.normal(stream_key, shape, jnp.float32) * width
    if len(cuts) > 0:
        entries = shard_levels(stream_key, shape, cuts, -0.22, 0.18) * entries
    return jnp.clip(entries, min=-bound, max=bound).astype(dtype)


def setup_inputs(seed: int = 0) -> dict:
    streams_of = jax.random.split(jax.random.key(seed), 10)
    layer_inputs = bell_draw(streams_of[0], (GROUPS, TOK_GRP, ROWS), 1.0, 6.0, ((0, 8), (1, 4)))
    key_cotangent = bell_draw(streams_of[1], (GROUPS, TOK_GRP, COLS), 0.015625, 0.099609375, ((0, 8), (1, 4)))
    key_weights = bell_draw(streams_of[2], (ROWS, COLS), ROWS ** -0.5, 0.125, ((0, 4),))
    outer_momentum = bell_draw(streams_of[3], (ROWS, COLS), 0.003, 0.02, ((0, 4),), jnp.float32)
    state_codes = set_ends(jax.random.randint(streams_of[4], (GROUPS, ROWS, COLS), 0, 256), jax.random.fold_in(streams_of[4], 1), 0, 255).astype(jnp.int32)
    first_row_max = jnp.clip(jnp.exp(math.log(2.0) - 2.9957323 * jax.random.uniform(streams_of[5], (GROUPS, ROWS), jnp.float32) ** shard_levels(streams_of[5], (GROUPS, ROWS), ((0, 8), (1, 4)), -0.2, 0.2)), 0.1, 2.0)
    first_col_max = jnp.clip(jnp.exp(math.log(2.0) - 2.9957323 * jax.random.uniform(streams_of[6], (GROUPS, COLS), jnp.float32) ** shard_levels(streams_of[6], (GROUPS, COLS), ((0, 8),), -0.2, 0.2)), 0.1, 2.0)
    second_row_max = jnp.clip(jnp.exp(math.log(4.0) - 3.6888794 * jax.random.uniform(streams_of[7], (GROUPS, ROWS), jnp.float32) ** shard_levels(streams_of[7], (GROUPS, ROWS), ((0, 8), (1, 4)), -0.2, 0.2)), 0.1, 4.0)
    second_col_max = jnp.clip(jnp.exp(math.log(4.0) - 3.6888794 * jax.random.uniform(streams_of[8], (GROUPS, COLS), jnp.float32) ** shard_levels(streams_of[8], (GROUPS, COLS), ((0, 8),), -0.2, 0.2)), 0.1, 4.0)
    return dict(layer_inputs=layer_inputs, key_cotangent=key_cotangent, key_weights=key_weights, outer_momentum=outer_momentum, state_codes=state_codes, first_row_max=first_row_max, first_col_max=first_col_max, second_row_max=second_row_max, second_col_max=second_col_max)


beta_one = 0.9
beta_two = 0.95
bias_one = 1.0 - 0.9 ** 10
bias_two = 1.0 - 0.95 ** 10
adam_eps = 1e-08
inner_rate = 0.01
weight_decay = 0.1
outer_rate = 0.7
outer_beta = 0.9
stat_eps = 1e-06

def adam_moments(gradient, packed_codes, first_rows, first_cols, second_rows, second_cols):
    first_code = (packed_codes // 16).astype(jnp.float32)
    second_code = (packed_codes % 16).astype(jnp.float32)
    first_old = jnp.minimum(first_rows[:, None], first_cols[None, :]) * (first_code - 7.5) / 7.5
    second_old = jnp.minimum(second_rows[:, None], second_cols[None, :]) * ((second_code + 1.0) / 16.0) ** 2
    first_new = beta_one * first_old + (1.0 - beta_one) * gradient
    second_new = beta_two * second_old + (1.0 - beta_two) * gradient * gradient
    return (first_new, second_new)

def pseudo_step(first_new, second_new, weights_float):
    update = first_new / bias_one / (jnp.sqrt(second_new / bias_two) + adam_eps)
    return inner_rate * (update + weight_decay * weights_float)

def reference(layer_inputs, key_cotangent, key_weights, outer_momentum, state_codes, first_row_max, first_col_max, second_row_max, second_col_max):
    weights_float = key_weights.astype(jnp.float32)

    def group_step(running, inputs):
        tokens, cotangent, packed_codes, first_rows, first_cols, second_rows, second_cols = inputs
        token_blocks = tokens.reshape(N_FSDP, TOK_DEV, ROWS)
        grad_blocks = cotangent.reshape(N_FSDP, TOK_DEV, COLS)

        def add_term(accum, pair):
            partial_term = lax.dot_general(pair[0], pair[1], (((0,), (0,)), ((), ())), preferred_element_type=jnp.float32)
            rounded = lax.optimization_barrier(partial_term.astype(jnp.bfloat16))
            return (accum + rounded.astype(jnp.float32), None)
        gradient, unused = lax.scan(add_term, jnp.zeros((ROWS, COLS), jnp.float32), (token_blocks, grad_blocks))
        first_new, second_new = adam_moments(gradient, packed_codes, first_rows, first_cols, second_rows, second_cols)
        pseudo = pseudo_step(first_new, second_new, weights_float)
        first_rmax = lax.optimization_barrier(jnp.max(jnp.abs(first_new), axis=1)) + stat_eps
        first_cmax = lax.optimization_barrier(jnp.max(jnp.abs(first_new), axis=0)) + stat_eps
        second_rmax = lax.optimization_barrier(jnp.max(second_new, axis=1)) + stat_eps
        second_cmax = lax.optimization_barrier(jnp.max(second_new, axis=0)) + stat_eps
        first_state = (first_new / jnp.minimum(first_rmax[:, None], first_cmax[None, :])).astype(jnp.bfloat16)
        second_state = (second_new / jnp.minimum(second_rmax[:, None], second_cmax[None, :])).astype(jnp.bfloat16)
        return (running + pseudo, (first_state, second_state, first_rmax, first_cmax, second_rmax, second_cmax))
    running, results = lax.scan(group_step, jnp.zeros((ROWS, COLS), jnp.float32), (layer_inputs, key_cotangent, state_codes, first_row_max, first_col_max, second_row_max, second_col_max))
    averaged = running / N_GRP
    new_momentum = outer_beta * outer_momentum + averaged
    new_weights = weights_float - outer_rate * (averaged + outer_beta * new_momentum)
    weights_half = new_weights.astype(jnp.bfloat16)

    def project(tokens):
        return jnp.dot(tokens, weights_half, preferred_element_type=jnp.float32).astype(jnp.bfloat16)
    next_keys = lax.map(project, layer_inputs)
    first_state, second_state, first_rmax, first_cmax, second_rmax, second_cmax = results
    return (new_weights, new_momentum, first_state, second_state, first_rmax, first_cmax, second_rmax, second_cmax, next_keys)
```

```python
import functools
import typing
import jax
import jax.numpy as jnp
from jax import lax
from jax.experimental import pallas as pl
from jax.experimental.pallas import tpu as pltpu
from jax.sharding import PartitionSpec as P

MESH = pl.DeviceIdType.MESH
f32, bf16 = jnp.float32, jnp.bfloat16
beta_one = 0.9
beta_two = 0.95
bias_one = 1.0 - 0.9**10
bias_two = 1.0 - 0.95**10
adam_eps = 1e-08
inner_rate = 0.01
weight_decay = 0.1
outer_rate = 0.7
outer_beta = 0.9
stat_eps = 1e-06
TILE = 16
UNIT = 128


class Stage(typing.NamedTuple):
    o: int
    R: int
    PR: int
    PC: int
    nc: int
    NP: int


def plan(rows, C, G):
    sizes = [UNIT] * (rows // UNIT - 1) + [UNIT // 2] * 2
    stages, o = [], 0
    for R in sizes:
        PR = max(TILE, R // G)
        nc = max(k for k in (1, 2, 3, 6) if k == 1 or (R // PR * k <= G and C % (128 * k) == 0))
        stages.append(Stage(o, R, PR, C // nc, nc, R // PR * nc))
        o += R
    return stages


def to_column(row):
    return jnp.broadcast_to(row, (128, row.shape[1])).T[:, :1]


def to_row(column):
    return jnp.broadcast_to(column, (column.shape[0], 128)).T[:1, :]


def kernel(
    n, G, stages,
    x_hbm, c_hbm, w_hbm, m_hbm, q_hbm, frm_hbm, fcm_hbm, srm_hbm, scm_hbm,
    o_w, o_m, o_fs, o_ss, o_frm, o_fcm, o_srm, o_scm, o_k,
    x, ct, w, m, q, frm, fcm, srm, scm,
    tb, rb, pb, rp, av, wf, fn, sn, acc, keys, fcol, scol, frn, srn, ca, cb, cmb,
    ld, ts, tr, ps, pr, as_, ar, gs, gr, ds, hs, hr, cs, cr,
):
    g = lax.axis_index("grp")
    z = lax.axis_index("fsdp")
    S = len(stages)
    rows, C = w.shape
    h = lax.rem(g, 2)
    mate = g + 1 - 2 * h
    other_z = lax.rem(z + 1, n)
    cut = rows - UNIT

    loads = [
        pltpu.make_async_copy(src, dst, ld.at[i])
        for i, (src, dst) in enumerate((
            (c_hbm, ct), (x_hbm, x), (frm_hbm, frm), (fcm_hbm, fcm), (srm_hbm, srm),
            (scm_hbm, scm), (q_hbm, q), (w_hbm, w), (m_hbm, m),
        ))
    ]
    barrier = pltpu.get_barrier_semaphore()
    for d in range(1, n):
        pl.semaphore_signal(
            barrier, inc=1, device_id=(g, lax.rem(z + d, n)), device_id_type=MESH
        )
    for d in range(1, G):
        pl.semaphore_signal(
            barrier, inc=1, device_id=(lax.rem(g + d, G), z), device_id_type=MESH
        )
    for load in loads:
        load.start()
    ca[...] = jnp.zeros_like(ca)
    cb[...] = jnp.zeros_like(cb)
    loads[0].wait()
    loads[1].wait()
    with jax.named_scope("barrier"):
        pl.semaphore_wait(barrier, G - 1 + n - 1)

    def term(c, s):
        st = stages[s]
        lead = st.o % UNIT
        columns = pl.ds(pl.multiple_of(c * rows + (st.o - lead), UNIT), UNIT)
        whole = lax.dot_general(
            x[:, columns], ct[...], (((0,), (0,)), ((), ())), preferred_element_type=f32
        )
        return whole[lead : lead + st.R]

    def block(s):
        return pl.ds(stages[s].o, stages[s].R)

    def move(s, c, slot, to):
        return pltpu.make_async_remote_copy(
            src_ref=tb.at[c, block(s)], dst_ref=rb.at[slot, block(s)], send_sem=ts.at[s, c],
            recv_sem=tr.at[s, slot], device_id=(g, to), device_id_type=MESH,
        )

    def stream(s):
        R = stages[s].R
        low = 2 * z < n

        def step(k, carry):
            nr = n - 1 - z
            right = jnp.where(low, jnp.where(k < nr, 1, 0), jnp.where(k < z, 0, 1)) == 1
            c = jnp.where(
                low, jnp.where(k < nr, n - 1 - k, k - nr), jnp.where(k < z, k, n - 1 - k + z)
            )
            to = jnp.where(right, z + 1, z - 1)
            slot = jnp.where(jnp.where(right, -1, z - 1) == c, n, c)
            acc[pl.ds(0, R), :] = term(c, s)

            @pl.when(jnp.where(right, z, n - 1 - z) == 0)
            def _():
                tb[c, block(s), :] = acc[pl.ds(0, R), :].astype(bf16)

            @pl.when(jnp.where(right, z, n - 1 - z) > 0)
            def _():
                move(s, c, c, other_z).wait_recv()
                tb[c, block(s), :] = (acc[pl.ds(0, R), :] + rb[c, block(s), :].astype(f32)).astype(bf16)

            move(s, c, slot, to).start()
            return carry

        lax.fori_loop(0, n - 1, step, 0)

    def place_of(s, p):
        st = stages[s]
        return (
            pl.ds(pl.multiple_of(st.o + p // st.nc * st.PR, TILE), st.PR),
            pl.ds(pl.multiple_of(lax.rem(p, st.nc) * st.PC, 128), st.PC),
        )

    def piece(s, p, to):
        st = stages[s]
        return pltpu.make_async_remote_copy(
            src_ref=pb.at[place_of(s, p)],
            dst_ref=rp.at[s, g, pl.ds(0, st.PR), pl.ds(0, st.PC)], send_sem=ps.at[s, p],
            recv_sem=pr.at[s, g], device_id=(to, z), device_id_type=MESH,
        )

    def piece_from(s, p):
        st = stages[s]
        here = rp.at[s, p, pl.ds(0, st.PR), pl.ds(0, st.PC)]
        return pltpu.make_async_remote_copy(
            src_ref=here, dst_ref=here, send_sem=ps.at[s, 0],
            recv_sem=pr.at[s, p], device_id=(mate, z), device_id_type=MESH,
        )

    def inner(s):
        st = stages[s]
        R = st.R
        acc[pl.ds(0, R), :] = term(z, s)

        @pl.when(z > 0)
        def _():
            move(s, z, z, other_z).wait_recv()
            acc[pl.ds(0, R), :] += rb[z, block(s), :].astype(f32)

        @pl.when(z < n - 1)
        def _():
            move(s, z, n, other_z).wait_recv()
            acc[pl.ds(0, R), :] += rb[n, block(s), :].astype(f32)

        def tile(i, carry):
            at = pl.multiple_of(i * TILE, TILE)
            place = pl.ds(pl.multiple_of(st.o + i * TILE, TILE), TILE)
            gradient = acc[pl.ds(at, TILE), :]
            codes = q[place, :]
            first_code = (codes >> 4).astype(f32)
            second_code = (codes & 15).astype(f32)
            second_code = second_code + 1.0
            first_new = (
                jnp.minimum(fcol[place, :], fcm[...]) * (first_code - 7.5)
                + (1.0 - beta_one) * gradient
            )
            second_new = (
                jnp.minimum(scol[place, :], scm[...]) * (second_code * second_code)
                + (1.0 - beta_two) * gradient * gradient
            )
            fn[place, :] = first_new
            sn[place, :] = second_new
            update = (first_new * (inner_rate / bias_one)) / (
                jnp.sqrt(second_new * (1.0 / bias_two)) + adam_eps
            )
            pseudo = update + (inner_rate * weight_decay) * w[place, :].astype(f32)
            pb[place, :] = pseudo.astype(bf16)
            size = jnp.abs(first_new)
            ca[...] = jnp.maximum(ca[...], size)
            cb[...] = jnp.maximum(cb[...], second_new)
            frn[place, :] = jnp.max(size, axis=1, keepdims=True) + stat_eps
            srn[place, :] = jnp.max(second_new, axis=1, keepdims=True) + stat_eps
            return carry

        lax.fori_loop(0, R // TILE, tile, 0)

        def send(d, carry):
            p = lax.rem(g + d, G)

            @pl.when(p < st.NP)
            def _():
                piece(s, p, p).start()

            return carry

        lax.fori_loop(1, G, send, 0)

    def share(s, p, to):
        return pltpu.make_async_remote_copy(
            src_ref=av.at[place_of(s, p)], dst_ref=av.at[place_of(s, p)], send_sem=as_.at[s, to],
            recv_sem=ar.at[s, p], device_id=(to, z), device_id_type=MESH,
        )

    def reduce(s):
        st = stages[s]
        top = (pl.ds(0, st.PR), pl.ds(0, st.PC))

        @pl.when(g < st.NP)
        def _():
            acc[top] = pb[place_of(s, g)].astype(f32)

            def add(d, carry):
                p = lax.rem(g + d, G)
                piece_from(s, p).wait_recv()
                acc[top] += rp[(s, p) + top].astype(f32)
                return carry

            lax.fori_loop(1, G, add, 0)
            av[place_of(s, g)] = (acc[top] * (1.0 / G)).astype(bf16)

            def send(d, carry):
                share(s, g, lax.rem(g + d, G)).start()
                return carry

            lax.fori_loop(1, G, send, 0)

    def half(s, which):
        st = stages[s]
        return pl.ds(pl.multiple_of(st.o + which * (st.R // 2), TILE), st.R // 2)

    def relay(s, c, way, to):
        part = half(s, h)
        return pltpu.make_async_remote_copy(
            src_ref=wf.at[c, part], dst_ref=wf.at[c, part], send_sem=gs.at[way, s, c],
            recv_sem=gr.at[s, c], device_id=(g, to), device_id_type=MESH,
        )

    def direct(to):
        part = half(S - 1, h)
        return pltpu.make_async_remote_copy(
            src_ref=wf.at[z, part], dst_ref=wf.at[z, part], send_sem=ds.at[to],
            recv_sem=gr.at[S - 1, z], device_id=(g, to), device_id_type=MESH,
        )

    def hand(s, c):
        part = half(s, h)
        return pltpu.make_async_remote_copy(
            src_ref=wf.at[c, part], dst_ref=wf.at[c, part], send_sem=hs.at[s, c],
            recv_sem=hr.at[s, c], device_id=(mate, z), device_id_type=MESH,
        )

    def hand_from(s, c):
        part = half(s, 1 - h)
        return pltpu.make_async_remote_copy(
            src_ref=wf.at[c, part], dst_ref=wf.at[c, part], send_sem=hs.at[s, c],
            recv_sem=hr.at[s, c], device_id=(mate, z), device_id_type=MESH,
        )

    def outer(s):
        st = stages[s]

        def wait(p, carry):
            @pl.when(p != g)
            def _():
                share(s, p, mate).wait_recv()

            return carry

        lax.fori_loop(0, st.NP, wait, 0)

        def tile(i, carry):
            place = pl.ds(pl.multiple_of(st.o + i * TILE, TILE), TILE)
            averaged = av[place, :].astype(f32)
            momentum = outer_beta * m[place, :] + averaged
            fresh = w[place, :].astype(f32) - outer_rate * (averaged + outer_beta * momentum)
            o_m[place, :] = momentum
            o_w[place, :] = fresh
            wf[z, place, :] = fresh.astype(bf16)
            return carry

        lax.fori_loop(0, st.R // TILE, tile, 0)
        if s < S - 1:
            @pl.when(z < n - 1)
            def _():
                relay(s, z, 0, z + 1).start()

            @pl.when(z > 0)
            def _():
                relay(s, z, 1, z - 1).start()
        else:
            for d in range(1, n):
                direct(lax.rem(z + d, n)).start()

    def from_left(s, c):
        relay(s, c, 0, other_z).wait_recv()

        @pl.when(z < n - 1)
        def _():
            relay(s, c, 0, z + 1).start()

        hand(s, c).start()

    def from_right(s, c):
        relay(s, c, 1, other_z).wait_recv()

        @pl.when(z > 0)
        def _():
            relay(s, c, 1, z - 1).start()

        hand(s, c).start()

    def hop_mid(s, j):
        @pl.when(z - j >= 1)
        def _():
            from_left(s, z - j)

        @pl.when(z + j <= n - 2)
        def _():
            from_right(s, z + j)

    def hop_end(s, j):
        @pl.when(z == j)
        def _():
            from_left(s, z - j)

        @pl.when(z == n - 1 - j)
        def _():
            from_right(s, z + j)

    @pl.when((z == 0) | (z == n - 1))
    def _():
        for s in range(S):
            with jax.named_scope(f"end{s}"):
                stream(s)

    for load in loads[2:]:
        load.wait()
    fcm[...] = fcm[...] * (beta_one / 7.5)
    scm[...] = scm[...] * (beta_two / 256.0)
    for o in range(0, rows, UNIT):
        part = pl.ds(o, UNIT)
        fcol[part, :] = to_column(frm[:, part] * (beta_one / 7.5))
        scol[part, :] = to_column(srm[:, part] * (beta_two / 256.0))

    def column_max(slot, to):
        return pltpu.make_async_remote_copy(
            src_ref=cmb.at[z], dst_ref=cmb.at[z], send_sem=cs.at[slot],
            recv_sem=cr.at[z], device_id=(g, to), device_id_type=MESH,
        )

    def column_max_from(c):
        return pltpu.make_async_remote_copy(
            src_ref=cmb.at[c], dst_ref=cmb.at[c], send_sem=cs.at[0],
            recv_sem=cr.at[c], device_id=(g, other_z), device_id_type=MESH,
        )

    done_mid = set()
    for s in range(S):
        @pl.when((z > 0) & (z < n - 1))
        def _():
            with jax.named_scope(f"stream{s}"):
                stream(s)
        if s >= 1:
            with jax.named_scope(f"reduce{s-1}"):
                reduce(s - 1)
        with jax.named_scope(f"inner{s}"):
            inner(s)
        if s == S - 1:
            cmb[z, pl.ds(0, 1), :] = jnp.max(ca[...], axis=0, keepdims=True)
            cmb[z, pl.ds(1, 1), :] = jnp.max(cb[...], axis=0, keepdims=True)
            for d in range(1, n):
                column_max(d, lax.rem(z + d, n)).start()
        if s >= 1:
            with jax.named_scope(f"outer{s-1}"):
                outer(s - 1)
        for t in range(S - 1):
            for j in range(1, n):
                if t + 1 + j == s:
                    done_mid.add((t, j))
                    with jax.named_scope(f"mid{t}{j}"):
                        hop_mid(t, j)

    def states():
        for c in range(1, n):
            column_max_from(lax.rem(z + c, n)).wait_recv()
        scales = jnp.max(cmb[...], axis=0) + stat_eps
        o_fcm[...] = scales[0:1]
        o_scm[...] = scales[1:2]
        fcm[...] = 1.0 / o_fcm[...]
        scm[...] = 1.0 / o_scm[...]

        def tile(i, carry):
            place = pl.ds(pl.multiple_of(i * TILE, TILE), TILE)
            first_inverse = jnp.maximum(1.0 / frn[place, :], fcm[...])
            second_inverse = jnp.maximum(1.0 / srn[place, :], scm[...])
            o_fs[place, :] = (fn[place, :] * first_inverse).astype(bf16)
            o_ss[place, :] = (sn[place, :] * second_inverse).astype(bf16)
            return carry

        lax.fori_loop(0, rows // TILE, tile, 0)
        for o in range(0, rows, UNIT):
            part = pl.ds(o, UNIT)
            o_frm[:, part] = to_row(frn[part, :])
            o_srm[:, part] = to_row(srn[part, :])

    def product(c, o, width):
        columns = pl.ds(pl.multiple_of(c * rows + o, UNIT), width)
        return jnp.dot(x[:, columns], wf[c, pl.ds(o, width), :], preferred_element_type=f32)

    def others(body):
        def step(j, carry):
            for c in (z - j, z + j):
                @pl.when((c >= 0) & (c < n))
                def _():
                    body(c)

            return carry

        lax.fori_loop(1, n, step, 0)

    def gather_early(c):
        for s in range(S - 2):
            hand_from(s, c).wait_recv()
        keys[...] += product(c, 0, cut)

    def own():
        if cut:
            keys[...] = product(z, 0, cut)
            keys[...] += product(z, cut, UNIT)
        else:
            keys[...] = product(z, cut, UNIT)

    todo = [(7.0, "reduce", functools.partial(reduce, S - 1)), (11.0, "outer", functools.partial(outer, S - 1))]
    todo += [(11.1, "own", own), (12.6, "states", states)]
    if cut:
        todo += [(14.5, "early", None)]
    for s in range(S - 1):
        for j in range(1, n):
            if (s, j) not in done_mid:
                when = 4.0 * j + 4.0 if s == S - 2 else 0.0
                todo.append((when, f"mid{s}{j}", functools.partial(hop_mid, s, j)))
            when = 1.7 + 2.1 * (s + 1) + 3.8 * (j - 1)
            todo.append((when, f"hop{s}{j}", functools.partial(hop_end, s, j)))
    late = [t for t in todo if t[1].startswith("hop") and t[0] > 13.0]
    for _, name, run in sorted((t for t in todo if t not in late), key=lambda t: t[0]):
        if name == "early":
            for _, lname, lrun in sorted(late, key=lambda t: t[0]):
                with jax.named_scope(lname):
                    lrun()
            with jax.named_scope("early"):
                others(gather_early)
        else:
            with jax.named_scope(name):
                run()
    if not cut:
        for _, _, run in sorted(late, key=lambda t: t[0]):
            run()

    def finish_from(c):
        part = half(S - 1, h)
        pltpu.make_async_remote_copy(
            src_ref=wf.at[c, part], dst_ref=wf.at[c, part], send_sem=ds.at[0],
            recv_sem=gr.at[S - 1, c], device_id=(g, other_z), device_id_type=MESH,
        ).wait_recv()
        hand(S - 1, c).start()

    with jax.named_scope("lastrecv"):
        others(finish_from)

    def gather_last(c):
        for s in (S - 2, S - 1):
            hand_from(s, c).wait_recv()
        keys[...] += product(c, cut, UNIT)

    with jax.named_scope("gatherlast"):
        others(gather_last)
    with jax.named_scope("okeys"):
        o_k[...] = keys[...].astype(bf16)

    with jax.named_scope("sends"):
        for s in range(S):
            def chunk(c, carry):
                @pl.when(c != z)
                def _():
                    move(s, c, c, other_z).wait_send()
                    hand(s, c).wait_send()

                if s < S - 1:
                    @pl.when((c <= z) & (z < n - 1))
                    def _():
                        relay(s, c, 0, other_z).wait_send()

                    @pl.when((c >= z) & (z > 0))
                    def _():
                        relay(s, c, 1, other_z).wait_send()

                return carry

            lax.fori_loop(0, n, chunk, 0)

            def plane(p, carry):
                @pl.when((p != g) & (p < stages[s].NP))
                def _():
                    piece(s, p, mate).wait_send()

                @pl.when((p != g) & (g < stages[s].NP))
                def _():
                    share(s, g, p).wait_send()

                return carry

            lax.fori_loop(0, G, plane, 0)
        for d in range(1, n):
            direct(lax.rem(z + d, n)).wait_send()
            column_max(d, other_z).wait_send()


def finish(*refs):
    k = (len(refs) - 1) // 2
    sems = refs[-1]
    copies = [
        pltpu.make_async_copy(src, dst, sems.at[i])
        for i, (src, dst) in enumerate(zip(refs[:k], refs[k:-1]))
    ]
    for copy in copies:
        copy.start()
    for copy in copies:
        copy.wait()


def local(x, ct, w, m, q, frm, fcm, srm, scm):
    n, G = lax.axis_size("fsdp"), lax.axis_size("grp")
    rows, C = w.shape
    T, K = x.shape[1:]
    stages = plan(rows, C, G)
    S = len(stages)
    PR = max(st.PR for st in stages)
    hbm = pl.BlockSpec(memory_space=pltpu.HBM)
    vmem = pl.BlockSpec(memory_space=pltpu.VMEM)
    dma = pltpu.SemaphoreType.DMA
    shape = jax.ShapeDtypeStruct
    outs = pl.pallas_call(
        functools.partial(kernel, n, G, stages),
        out_shape=(
            pltpu.VMEM((rows, C), f32), pltpu.VMEM((rows, C), f32),
            pltpu.VMEM((rows, C), bf16), pltpu.VMEM((rows, C), bf16),
            pltpu.VMEM((1, rows), f32), pltpu.VMEM((1, C), f32),
            pltpu.VMEM((1, rows), f32), pltpu.VMEM((1, C), f32),
            pltpu.VMEM((T, C), bf16),
        ),
        in_specs=[hbm] * 9,
        out_specs=(vmem,) * 9,
        scratch_shapes=[
            pltpu.VMEM((T, K), bf16), pltpu.VMEM((T, C), bf16), pltpu.VMEM((rows, C), bf16),
            pltpu.VMEM((rows, C), f32), pltpu.VMEM((rows, C), jnp.int32),
            pltpu.VMEM((1, rows), f32), pltpu.VMEM((1, C), f32),
            pltpu.VMEM((1, rows), f32), pltpu.VMEM((1, C), f32),
            pltpu.VMEM((n, rows, C), bf16), pltpu.VMEM((n + 1, rows, C), bf16),
            pltpu.VMEM((rows, C), bf16), pltpu.VMEM((S, G, PR, C), bf16),
            pltpu.VMEM((rows, C), bf16), pltpu.VMEM((n, rows, C), bf16),
            pltpu.VMEM((rows, C), f32), pltpu.VMEM((rows, C), f32),
            pltpu.VMEM((UNIT, C), f32), pltpu.VMEM((T, C), f32),
            pltpu.VMEM((rows, 1), f32), pltpu.VMEM((rows, 1), f32),
            pltpu.VMEM((rows, 1), f32), pltpu.VMEM((rows, 1), f32),
            pltpu.VMEM((TILE, C), f32), pltpu.VMEM((TILE, C), f32), pltpu.VMEM((n, 2, C), f32),
            dma((9,)), dma((S, n)), dma((S, n + 1)), dma((S, G)), dma((S, G)),
            dma((S, G)), dma((S, G)), dma((2, S, n)), dma((S, n)), dma((n,)),
            dma((S, n)), dma((S, n)), dma((n,)), dma((n,)),
        ],
        compiler_params=pltpu.CompilerParams(
            collective_id=0, has_side_effects=True, vmem_limit_bytes=54 * 1024 * 1024
        ),
    )(x[0], ct[0], w, m, q[0], frm, fcm, srm, scm)
    done = pl.pallas_call(
        finish,
        out_shape=tuple(shape(a.shape, a.dtype) for a in outs),
        in_specs=(vmem,) * 9,
        out_specs=(hbm,) * 9,
        scratch_shapes=[dma((9,))],
        compiler_params=pltpu.CompilerParams(vmem_limit_bytes=8 * 1024 * 1024),
    )(*outs)
    new_w, new_m, fs, ss, nfr, nfc, nsr, nsc, keys = done
    return new_w, new_m, fs[None], ss[None], nfr, nfc, nsr, nsc, keys[None]


def solution(mesh):
    return jax.shard_map(
        local,
        mesh=mesh,
        in_specs=(
            P("grp", "fsdp", None), P("grp", "fsdp", None), P("fsdp", None), P("fsdp", None),
            P("grp", "fsdp", None), P("grp", "fsdp"), P("grp", None), P("grp", "fsdp"),
            P("grp", None),
        ),
        out_specs=(
            P("fsdp", None), P("fsdp", None), P("grp", "fsdp", None), P("grp", "fsdp", None),
            P("grp", "fsdp"), P("grp", None), P("grp", "fsdp"), P("grp", None),
            P("grp", "fsdp", None),
        ),
        check_vma=False,
    )
```

```python
import functools
import typing
import jax
import jax.numpy as jnp
from jax import lax
from jax.experimental import pallas as pl
from jax.experimental.pallas import tpu as pltpu
from jax.sharding import PartitionSpec as P

MESH = pl.DeviceIdType.MESH
f32, bf16 = jnp.float32, jnp.bfloat16
beta_one = 0.9
beta_two = 0.95
bias_one = 1.0 - 0.9**10
bias_two = 1.0 - 0.95**10
adam_eps = 1e-08
inner_rate = 0.01
weight_decay = 0.1
outer_rate = 0.7
outer_beta = 0.9
stat_eps = 1e-06
TILE = 16
UNIT = 128
LAST = [64, 64]
NEAR = 2

class Stage(typing.NamedTuple):
    o: int
    R: int
    PR: int
    PC: int
    nc: int
    NP: int


def plan(rows, C, G):
    sizes = [UNIT] * (rows // UNIT - 1) + LAST
    stages, o = [], 0
    for R in sizes:
        PR = max(TILE, R // G)
        nc = max(k for k in (1, 2, 3, 6) if k == 1 or (R // PR * k <= G and C % (128 * k) == 0))
        stages.append(Stage(o, R, PR, C // nc, nc, R // PR * nc))
        o += R
    return stages


def to_column(row):
    return jnp.broadcast_to(row, (128, row.shape[1])).T


def kernel(
    n, G, stages,
    x_hbm, c_hbm, w_hbm, m_hbm, q_hbm, frm_hbm, fcm_hbm, srm_hbm, scm_hbm,
    o_w, o_m, o_fs, o_ss, o_frm, o_fcm, o_srm, o_scm, o_k,
    x, ct, w, m, q, frm, fcm, srm, scm,
    tb, rb, pb, rp, av, wo, wf, fn, sn, acc, keys, fcol, scol, frn, srn, ca, cb, cmb,
    ld, ts, tr, ps, pr, zs, zf, gr, hs, hr, hm, cs, cr,
):
    g = lax.axis_index("grp")
    z = lax.axis_index("fsdp")
    S = len(stages)
    rows, C = w.shape
    h = lax.rem(g, 2)
    mate = g + 1 - 2 * h
    other_z = lax.rem(z + 1, n)
    cut = rows - UNIT
    lanes = [pl.ds(k, 128) for k in range(0, C, 128)]

    loads = [
        pltpu.make_async_copy(src, dst, ld.at[i])
        for i, (src, dst) in enumerate((
            (c_hbm, ct), (x_hbm, x), (frm_hbm, frm), (fcm_hbm, fcm), (srm_hbm, srm),
            (scm_hbm, scm), (q_hbm, q), (w_hbm, w), (m_hbm, m),
        ))
    ]
    barrier = pltpu.get_barrier_semaphore()
    for d in range(1, n):
        pl.semaphore_signal(
            barrier, inc=1, device_id=(g, lax.rem(z + d, n)), device_id_type=MESH
        )
    for d in range(1, G):
        pl.semaphore_signal(
            barrier, inc=1, device_id=(lax.rem(g + d, G), z), device_id_type=MESH
        )
    for load in loads:
        load.start()
    ca[...] = jnp.zeros_like(ca)
    cb[...] = jnp.zeros_like(cb)
    loads[0].wait()
    loads[1].wait()
    with jax.named_scope("barrier"):
        pl.semaphore_wait(barrier, G - 1 + n - 1)

    def term(c, s):
        st = stages[s]
        lead = st.o % UNIT
        columns = pl.ds(pl.multiple_of(c * rows + (st.o - lead), UNIT), UNIT)
        whole = lax.dot_general(
            x[:, columns], ct[...], (((0,), (0,)), ((), ())), preferred_element_type=f32
        )
        return whole[lead : lead + st.R]

    def block(s):
        return pl.ds(stages[s].o, stages[s].R)

    def move(s, c, slot, to):
        return pltpu.make_async_remote_copy(
            src_ref=tb.at[c, block(s)], dst_ref=rb.at[slot, block(s)], send_sem=ts,
            recv_sem=tr.at[s, slot], device_id=(g, to), device_id_type=MESH,
        )

    def forward(s, k):
        R = stages[s].R
        low = 2 * z < n
        nr = n - 1 - z
        right = jnp.where(low, jnp.where(k < nr, 1, 0), jnp.where(k < z, 0, 1)) == 1
        c = jnp.where(
            low, jnp.where(k < nr, n - 1 - k, k - nr), jnp.where(k < z, k, n - 1 - k + z)
        )
        to = jnp.where(right, z + 1, z - 1)
        slot = jnp.where(jnp.where(right, -1, z - 1) == c, n, c)
        acc[pl.ds(0, R), :] = term(c, s)

        @pl.when(jnp.where(right, z, n - 1 - z) == 0)
        def _():
            tb[c, block(s), :] = acc[pl.ds(0, R), :].astype(bf16)

        @pl.when(jnp.where(right, z, n - 1 - z) > 0)
        def _():
            move(s, c, c, other_z).wait_recv()
            tb[c, block(s), :] = (acc[pl.ds(0, R), :] + rb[c, block(s), :].astype(f32)).astype(bf16)

        move(s, c, slot, to).start()

    def between(body):
        @pl.when((z > 0) & (z < n - 1))
        def _():
            body()

    def at_ends(body):
        @pl.when((z == 0) | (z == n - 1))
        def _():
            body()

    def place_of(s, p):
        st = stages[s]
        return (
            pl.ds(pl.multiple_of(st.o + p // st.nc * st.PR, TILE), st.PR),
            pl.ds(pl.multiple_of(lax.rem(p, st.nc) * st.PC, 128), st.PC),
        )

    def piece(s, p, to):
        st = stages[s]
        return pltpu.make_async_remote_copy(
            src_ref=pb.at[place_of(s, p)],
            dst_ref=rp.at[s, g, pl.ds(0, st.PR), pl.ds(0, st.PC)], send_sem=ps.at[s],
            recv_sem=pr.at[s], device_id=(to, z), device_id_type=MESH,
        )

    def pieces(s, k, sem):
        st = stages[s]
        several = rp.at[s, pl.ds(0, k), pl.ds(0, st.PR), pl.ds(0, st.PC)]
        return pltpu.make_async_copy(several, several, sem)

    def pieces_but_own(s, sem, count=None):
        st = stages[s]
        count = st.NP if count is None else count

        @pl.when(g < st.NP)
        def _():
            pieces(s, count - 1, sem).wait()

        if st.NP < G:
            @pl.when(g >= st.NP)
            def _():
                pieces(s, count, sem).wait()

    def inner(s):
        st = stages[s]
        R = st.R
        acc[pl.ds(0, R), :] = term(z, s)

        @pl.when(z > 0)
        def _():
            move(s, z, z, other_z).wait_recv()
            acc[pl.ds(0, R), :] += rb[z, block(s), :].astype(f32)

        @pl.when(z < n - 1)
        def _():
            move(s, z, n, other_z).wait_recv()
            acc[pl.ds(0, R), :] += rb[n, block(s), :].astype(f32)

        def tile(i, carry):
            at = pl.ds(pl.multiple_of(i * TILE, TILE), TILE)
            place = pl.ds(pl.multiple_of(st.o + i * TILE, TILE), TILE)
            first_row, second_row = fcol[place, :], scol[place, :]
            first_top, second_top = None, None
            for lane in lanes:
                gradient = acc[at, lane]
                codes = q[place, lane]
                first_code = (codes >> 4).astype(f32)
                second_code = (codes & 15).astype(f32) + 1.0
                first_new = (
                    jnp.minimum(first_row, fcm[:, lane]) * (first_code - 7.5)
                    + (1.0 - beta_one) * gradient
                )
                second_new = (
                    jnp.minimum(second_row, scm[:, lane]) * (second_code * second_code)
                    + (1.0 - beta_two) * gradient * gradient
                )
                fn[place, lane] = first_new
                sn[place, lane] = second_new
                update = (first_new * (inner_rate / bias_one)) / (
                    jnp.sqrt(second_new * (1.0 / bias_two)) + adam_eps
                )
                pseudo = update + (inner_rate * weight_decay) * w[place, lane].astype(f32)
                pb[place, lane] = pseudo.astype(bf16)
                size = jnp.abs(first_new)
                ca[:, lane] = jnp.maximum(ca[:, lane], size)
                cb[:, lane] = jnp.maximum(cb[:, lane], second_new)
                first_top = size if first_top is None else jnp.maximum(first_top, size)
                second_top = second_new if second_top is None else jnp.maximum(second_top, second_new)
            frn[place, :] = first_top
            srn[place, :] = second_top
            return carry

        lax.fori_loop(0, R // TILE, tile, 0)

        def send(d, carry):
            p = lax.rem(g + d, G)

            @pl.when(p < st.NP)
            def _():
                piece(s, p, p).start()

            return carry

        lax.fori_loop(1, G, send, 0)

    def plane_copy(s, c, p, to, sem):
        here = (av if c is None else wf.at[c]).at[place_of(s, p)]
        key = z if c is None else c
        return pltpu.make_async_remote_copy(
            src_ref=here, dst_ref=here, send_sem=hs.at[s, key],
            recv_sem=sem.at[s, key], device_id=(to, z), device_id_type=MESH,
        )

    def share(s, c):
        def send(d, carry):
            plane_copy(s, c, g, lax.rem(g + 2 * d, G), hr).start()
            return carry

        lax.fori_loop(1, G // 2, send, 0)
        plane_copy(s, c, g, mate, hm).start()

    def hand(s, c):
        st = stages[s]
        pieces_but_own(s, hr.at[s, z if c is None else c], st.NP // 2)

        def send(d, carry):
            p = lax.rem(g + 2 * d, G)

            @pl.when(p < st.NP)
            def _():
                plane_copy(s, c, p, mate, hm).start()

            return carry

        lax.fori_loop(1, G // 2, send, 0)

    def arrived(s, c):
        pieces(s, stages[s].NP // 2, hm.at[s, z if c is None else c]).wait()

    def reduce(s):
        st = stages[s]
        top = (pl.ds(0, st.PR), pl.ds(0, st.PC))

        @pl.when(g < st.NP)
        def _():
            pieces(s, G - 1, pr.at[s]).wait()
            acc[top] = pb[place_of(s, g)].astype(f32)

            def add(d, carry):
                acc[top] += rp[(s, lax.rem(g + d, G)) + top].astype(f32)
                return carry

            lax.fori_loop(1, G, add, 0)
            averaged = (acc[top] * (1.0 / G)).astype(bf16)
            av[place_of(s, g)] = averaged
            averaged = averaged.astype(f32)
            momentum = outer_beta * m[place_of(s, g)] + averaged
            fresh = w[place_of(s, g)].astype(f32) - outer_rate * (averaged + outer_beta * momentum)
            wo[(s,) + top] = fresh.astype(bf16)

            if s < NEAR:
                between(lambda: to_planes(s))

                @pl.when(z == 0)
                def _():
                    own_piece(s, z + 1).start()

                @pl.when(z == n - 1)
                def _():
                    own_piece(s, z - 1).start()
            else:
                to_planes(s)

            share(s, None)

    def own_piece(s, to):
        st = stages[s]
        return pltpu.make_async_remote_copy(
            src_ref=wo.at[s, pl.ds(0, st.PR), pl.ds(0, st.PC)],
            dst_ref=wf.at[(z,) + place_of(s, g)], send_sem=zs.at[s],
            recv_sem=gr.at[s, z], device_id=(g, to), device_id_type=MESH,
        )

    def to_planes(s):
        for d in range(1, n):
            own_piece(s, lax.rem(z + d, n)).start()

    def passed(s, c, to):
        here = wf.at[(c,) + place_of(s, g)]
        return pltpu.make_async_remote_copy(
            src_ref=here, dst_ref=here, send_sem=zf.at[s],
            recv_sem=gr.at[s, c], device_id=(g, to), device_id_type=MESH,
        )

    def spread(s, c):
        @pl.when(g < stages[s].NP)
        def _():
            passed(s, c, other_z).wait_recv()
            if s < NEAR:
                @pl.when((c == 0) & (z == 1))
                def _():
                    for to in range(2, n):
                        passed(s, c, to).start()

                @pl.when((c == n - 1) & (z == n - 2))
                def _():
                    for to in range(n - 2):
                        passed(s, c, to).start()

            share(s, c)

    def over_mid(body, s):
        def step(c, carry):
            @pl.when(c != z)
            def _():
                body(s, c)

            return carry

        lax.fori_loop(1, n - 1, step, 0)

    def over_near(body, s):
        if n > 2:
            @pl.when(z == 1)
            def _():
                body(s, 0)

            @pl.when(z == n - 2)
            def _():
                body(s, n - 1)

    def over_far(body, s):
        @pl.when((z != 0) & ((z != 1) | (n == 2)))
        def _():
            body(s, 0)

        @pl.when((z != n - 1) & ((z != n - 2) | (n == 2)))
        def _():
            body(s, n - 1)

    def outer(s):
        st = stages[s]
        arrived(s, None)

        def tile(i, carry):
            place = pl.ds(pl.multiple_of(st.o + i * TILE, TILE), TILE)
            averaged = av[place, :].astype(f32)
            momentum = outer_beta * m[place, :] + averaged
            fresh = w[place, :].astype(f32) - outer_rate * (averaged + outer_beta * momentum)
            o_m[place, :] = momentum
            o_w[place, :] = fresh
            wf[z, place, :] = fresh.astype(bf16)
            return carry

        lax.fori_loop(0, st.R // TILE, tile, 0)
    def turn(s, k):
        at = s + k / max(1, n - 2)
        return at - 0.99 if s == S - 1 and k < n - 2 else at

    order = sorted((turn(s, k), k, s) for s in range(S) for k in range(n - 1))

    def send_group(first, last):
        @at_ends
        def _():
            for at, k, s in order:
                if first <= at < last:
                    forward(s, k)

    done = set()

    def once(name, body, *key):
        if min(key[:1]) >= 0 and (name, key) not in done:
            done.add((name, key))
            with jax.named_scope(f"{name}{'_'.join(str(k) for k in key if isinstance(k, int))}"):
                body()

    def do(over, body, t):
        once(body.__name__ + over.__name__[4:], lambda: over(body, t), t)

    paced = S > 3
    send_group(0, 2 if paced else S + 1)

    for load in loads[2:]:
        load.wait()
    fcm[...] = fcm[...] * (beta_one / 7.5)
    scm[...] = scm[...] * (beta_two / 256.0)
    for o in range(0, rows, UNIT):
        part = pl.ds(o, UNIT)
        fcol[part, :] = to_column(frm[:, part] * (beta_one / 7.5))
        scol[part, :] = to_column(srm[:, part] * (beta_two / 256.0))

    def column_max(slot, to):
        return pltpu.make_async_remote_copy(
            src_ref=cmb.at[z], dst_ref=cmb.at[z], send_sem=cs,
            recv_sem=cr, device_id=(g, to), device_id_type=MESH,
        )

    def all_column_max(sem):
        several = cmb.at[pl.ds(0, n - 1)]
        return pltpu.make_async_copy(several, several, sem)

    def forward_rest(s):
        def step(k, carry):
            forward(s, k)
            return carry

        lax.fori_loop(1, n - 1, step, 0)

    def row_max(s):
        part = block(s)
        first = jnp.max(frn[part, :], axis=1, keepdims=True) + stat_eps
        second = jnp.max(srn[part, :], axis=1, keepdims=True) + stat_eps
        frn[part, :] = jnp.broadcast_to(first, (stages[s].R, 128))
        srn[part, :] = jnp.broadcast_to(second, (stages[s].R, 128))

    def rows_out():
        for o in range(0, rows, UNIT):
            part = pl.ds(o, UNIT)
            o_frm[:, part] = frn[part, :].T[:1, :]
            o_srm[:, part] = srn[part, :].T[:1, :]

    for s in range(S):
        last = s == S - 1
        with jax.named_scope(f"fwA{s}"):
            between(functools.partial(forward, s, 0))
        if last:
            with jax.named_scope(f"fwB{s}"):
                between(functools.partial(forward_rest, s))
        if s >= 1:
            with jax.named_scope(f"inner{s-1}"):
                inner(s - 1)
        if last:
            break
        do(over_mid, spread, s - 2)
        if s - 2 < NEAR:
            do(over_near, spread, s - 2)
        if s - 3 < NEAR:
            do(over_far, spread, s - 3)
        once("handav", lambda: hand(s - 2, None), s - 2)
        do(over_mid, hand, s - 3)
        if s - 3 < NEAR:
            do(over_near, hand, s - 3)
        if s - 4 < NEAR:
            do(over_far, hand, s - 4)
        if s >= 1:
            row_max(s - 1)
        with jax.named_scope(f"fwB{s}"):
            between(functools.partial(forward_rest, s))
        once("reduce", lambda: reduce(s - 1), s - 1)
        once("outer", lambda: outer(s - 2), s - 2)
        if paced and s in (1, 2):
            with jax.named_scope(f"group{s+1}"):
                send_group(s + 1, s + 2 if s == 1 else S + 1)

    def last_inner():
        inner(S - 1)
        cmb[z, pl.ds(0, 1), :] = jnp.max(ca[...], axis=0, keepdims=True)
        cmb[z, pl.ds(1, 1), :] = jnp.max(cb[...], axis=0, keepdims=True)
        for d in range(1, n):
            column_max(d, lax.rem(z + d, n)).start()

    def states():
        all_column_max(cr).wait()
        scales = jnp.max(cmb[...], axis=0) + stat_eps
        o_fcm[...] = scales[0:1]
        o_scm[...] = scales[1:2]
        fcm[...] = 1.0 / o_fcm[...]
        scm[...] = 1.0 / o_scm[...]

        def tile(i, carry):
            place = pl.ds(pl.multiple_of(i * TILE, TILE), TILE)
            first_row, second_row = 1.0 / frn[place, :], 1.0 / srn[place, :]
            for lane in lanes:
                o_fs[place, lane] = (fn[place, lane] * jnp.maximum(first_row, fcm[:, lane])).astype(bf16)
                o_ss[place, lane] = (sn[place, lane] * jnp.maximum(second_row, scm[:, lane])).astype(bf16)
            return carry

        lax.fori_loop(0, rows // TILE, tile, 0)

    def product(c, o, width):
        columns = pl.ds(pl.multiple_of(c * rows + o, UNIT), width)
        return jnp.dot(x[:, columns], wf[c, pl.ds(o, width), :], preferred_element_type=f32)

    def others(body):
        def step(j, carry):
            for c in (z - j, z + j):
                @pl.when((c >= 0) & (c < n))
                def _():
                    body(c)

            return carry

        lax.fori_loop(1, n, step, 0)

    def gather_early(c):
        for s in range(S - 2):
            arrived(s, c)
        keys[...] += product(c, 0, cut)

    def gather_mid(c):
        @pl.when((c > 0) & (c < n - 1))
        def _():
            gather_early(c)

    def gather_end(c):
        @pl.when((c == 0) | (c == n - 1))
        def _():
            gather_early(c)

    def own():
        if cut:
            keys[...] = product(z, 0, cut)
        else:
            keys[...] = jnp.zeros_like(keys)

    def run(name, body):
        with jax.named_scope(name):
            body()

    everywhere = (over_mid, over_near, over_far)
    run("lastinner", last_inner)
    once("reduce", lambda: reduce(S - 2), S - 2)
    row_max(S - 2)
    row_max(S - 1)
    run("rowsout", rows_out)
    for t in range(S - 2):
        for over in everywhere:
            do(over, spread, t)
    for t in range(S - 2):
        once("handav", functools.partial(hand, t, None), t)
        once("outer", functools.partial(outer, t), t)
    run("own", own)
    once("reduce", lambda: reduce(S - 1), S - 1)
    for over in everywhere:
        do(over, spread, S - 2)
    for t in range(S - 2):
        for over in everywhere:
            do(over, hand, t)
    once("handav", lambda: hand(S - 2, None), S - 2)
    run("states", states)
    if cut:
        run("gmid", functools.partial(others, gather_mid))
    for over in everywhere:
        do(over, spread, S - 1)
    for over in everywhere:
        do(over, hand, S - 2)
    once("outer", lambda: outer(S - 2), S - 2)
    once("handav", lambda: hand(S - 1, None), S - 1)
    if cut:
        run("gend", functools.partial(others, gather_end))
    once("outer", lambda: outer(S - 1), S - 1)
    for over in everywhere:
        do(over, hand, S - 1)

    def last_pieces(c):
        for s in (S - 2, S - 1):
            arrived(s, c)

    run("lastpieces", functools.partial(others, last_pieces))

    def last_product():
        TT = UNIT

        def tile(i, carry):
            tokens = pl.ds(pl.multiple_of(i * TT, TT), TT)
            total = keys[tokens, :]
            for c in range(n):
                total += jnp.dot(
                    x[tokens, pl.ds(c * rows + cut, UNIT)], wf[c, pl.ds(cut, UNIT), :],
                    preferred_element_type=f32,
                )
            o_k[tokens, :] = total.astype(bf16)
            return carry

        lax.fori_loop(0, x.shape[0] // TT, tile, 0)

    run("lastprod", last_product)

    def sends():
        chunks = tb.at[pl.ds(0, n - 1)]
        pltpu.make_async_copy(chunks, chunks, ts).wait()

        for s in range(S):
            pieces_but_own(s, ps.at[s])

        def chunk(c, carry):
            for s in range(S):
                half = stages[s].NP // 2

                @pl.when(g < stages[s].NP)
                def _():
                    pieces(s, G // 2 + half - 1, hs.at[s, c]).wait()

                if stages[s].NP < G:
                    @pl.when(g >= stages[s].NP)
                    def _():
                        pieces(s, half, hs.at[s, c]).wait()

            return carry

        lax.fori_loop(0, n, chunk, 0)
        for s in range(S):
            @pl.when(g < stages[s].NP)
            def _():
                if s >= NEAR:
                    pieces(s, n - 1, zs.at[s]).wait()
                else:
                    between(lambda: pieces(s, n - 1, zs.at[s]).wait())
                    at_ends(lambda: pieces(s, 1, zs.at[s]).wait())
                    if n > 3:
                        @pl.when((z == 1) | (z == n - 2))
                        def _():
                            pieces(s, n - 2, zf.at[s]).wait()

        all_column_max(cs).wait()

    run("sends", sends)


def finish(*refs):
    k = (len(refs) - 1) // 2
    sems = refs[-1]
    copies = [
        pltpu.make_async_copy(src, dst, sems.at[i])
        for i, (src, dst) in enumerate(zip(refs[:k], refs[k:-1]))
    ]
    for copy in copies:
        copy.start()
    for copy in copies:
        copy.wait()


def local(x, ct, w, m, q, frm, fcm, srm, scm):
    n, G = lax.axis_size("fsdp"), lax.axis_size("grp")
    rows, C = w.shape
    T, K = x.shape[1:]
    stages = plan(rows, C, G)
    S = len(stages)
    PR = max(st.PR for st in stages)
    hbm = pl.BlockSpec(memory_space=pltpu.HBM)
    vmem = pl.BlockSpec(memory_space=pltpu.VMEM)
    dma = pltpu.SemaphoreType.DMA
    shape = jax.ShapeDtypeStruct
    outs = pl.pallas_call(
        functools.partial(kernel, n, G, stages),
        out_shape=(
            pltpu.VMEM((rows, C), f32), pltpu.VMEM((rows, C), f32),
            pltpu.VMEM((rows, C), bf16), pltpu.VMEM((rows, C), bf16),
            pltpu.VMEM((1, rows), f32), pltpu.VMEM((1, C), f32),
            pltpu.VMEM((1, rows), f32), pltpu.VMEM((1, C), f32),
            pltpu.VMEM((T, C), bf16),
        ),
        in_specs=[hbm] * 9,
        out_specs=(vmem,) * 9,
        scratch_shapes=[
            pltpu.VMEM((T, K), bf16), pltpu.VMEM((T, C), bf16), pltpu.VMEM((rows, C), bf16),
            pltpu.VMEM((rows, C), f32), pltpu.VMEM((rows, C), jnp.int32),
            pltpu.VMEM((1, rows), f32), pltpu.VMEM((1, C), f32),
            pltpu.VMEM((1, rows), f32), pltpu.VMEM((1, C), f32),
            pltpu.VMEM((n, rows, C), bf16), pltpu.VMEM((n + 1, rows, C), bf16),
            pltpu.VMEM((rows, C), bf16), pltpu.VMEM((S, G, PR, C), bf16),
            pltpu.VMEM((rows, C), bf16), pltpu.VMEM((S, PR, C), bf16), pltpu.VMEM((n, rows, C), bf16),
            pltpu.VMEM((rows, C), f32), pltpu.VMEM((rows, C), f32),
            pltpu.VMEM((UNIT, C), f32), pltpu.VMEM((T, C), f32),
            pltpu.VMEM((rows, 128), f32), pltpu.VMEM((rows, 128), f32),
            pltpu.VMEM((rows, 128), f32), pltpu.VMEM((rows, 128), f32),
            pltpu.VMEM((TILE, C), f32), pltpu.VMEM((TILE, C), f32), pltpu.VMEM((n, 2, C), f32),
            dma((9,)), dma, dma((S, n + 1)), dma((S,)), dma((S,)), dma((S,)), dma((S,)),
            dma((S, n)), dma((S, n)), dma((S, n)), dma((S, n)), dma, dma,
        ],
        compiler_params=pltpu.CompilerParams(
            collective_id=0, has_side_effects=True, vmem_limit_bytes=54 * 1024 * 1024
        ),
    )(x[0], ct[0], w, m, q[0], frm, fcm, srm, scm)
    done = pl.pallas_call(
        finish,
        out_shape=tuple(shape(a.shape, a.dtype) for a in outs),
        in_specs=(vmem,) * 9,
        out_specs=(hbm,) * 9,
        scratch_shapes=[dma((9,))],
        compiler_params=pltpu.CompilerParams(vmem_limit_bytes=8 * 1024 * 1024),
    )(*outs)
    new_w, new_m, fs, ss, nfr, nfc, nsr, nsc, keys = done
    return new_w, new_m, fs[None], ss[None], nfr, nfc, nsr, nsc, keys[None]


def solution(mesh):
    return jax.shard_map(
        local,
        mesh=mesh,
        in_specs=(
            P("grp", "fsdp", None), P("grp", "fsdp", None), P("fsdp", None), P("fsdp", None),
            P("grp", "fsdp", None), P("grp", "fsdp"), P("grp", None), P("grp", "fsdp"),
            P("grp", None),
        ),
        out_specs=(
            P("fsdp", None), P("fsdp", None), P("grp", "fsdp", None), P("grp", "fsdp", None),
            P("grp", "fsdp"), P("grp", None), P("grp", "fsdp"), P("grp", None),
            P("grp", "fsdp", None),
        ),
        check_vma=False,
    )
```

```python
import functools
import typing
import jax
import jax.numpy as jnp
from jax import lax
from jax.experimental import pallas as pl
from jax.experimental.pallas import tpu as pltpu
from jax.sharding import PartitionSpec as P

MESH = pl.DeviceIdType.MESH
f32, bf16 = jnp.float32, jnp.bfloat16
beta_one = 0.9
beta_two = 0.95
bias_one = 1.0 - 0.9**10
bias_two = 1.0 - 0.95**10
adam_eps = 1e-08
inner_rate = 0.01
weight_decay = 0.1
outer_rate = 0.7
outer_beta = 0.9
stat_eps = 1e-06
TILE = 16
UNIT = 128
LAST = [64, 64]
NEAR = 2

class Stage(typing.NamedTuple):
    o: int
    R: int
    PR: int
    PC: int
    nc: int
    NP: int


def plan(rows, C, G):
    sizes = [UNIT] * (rows // UNIT - 1) + LAST
    stages, o = [], 0
    for R in sizes:
        PR = max(TILE, R // G)
        nc = max(k for k in (1, 2, 3, 6) if k == 1 or (R // PR * k <= G and C % (128 * k) == 0))
        stages.append(Stage(o, R, PR, C // nc, nc, R // PR * nc))
        o += R
    return stages


def to_column(row):
    return jnp.broadcast_to(row, (128, row.shape[1])).T


def kernel(
    n, G, stages,
    x_hbm, c_hbm, w_hbm, m_hbm, q_hbm, frm_hbm, fcm_hbm, srm_hbm, scm_hbm,
    o_w, o_m, o_fs, o_ss, o_frm, o_fcm, o_srm, o_scm, o_k,
    x, ct, w, m, q, frm, fcm, srm, scm,
    tb, rb, pb, rp, av, wo, wf, fn, sn, acc, keys, fcol, scol, frn, srn, ca, cb, cmb,
    ld, ts, tr, ps, pr, zs, zf, gr, hs, hr, hm, cs, cr,
):
    g = lax.axis_index("grp")
    z = lax.axis_index("fsdp")
    S = len(stages)
    rows, C = w.shape
    h = lax.rem(g, 2)
    mate = g + 1 - 2 * h
    other_z = lax.rem(z + 1, n)
    cut = rows - UNIT
    held = S - 3
    lanes = [pl.ds(k, 128) for k in range(0, C, 128)]

    loads = [
        pltpu.make_async_copy(src, dst, ld.at[i])
        for i, (src, dst) in enumerate((
            (c_hbm, ct), (x_hbm, x), (frm_hbm, frm), (fcm_hbm, fcm), (srm_hbm, srm),
            (scm_hbm, scm), (q_hbm, q), (w_hbm, w), (m_hbm, m),
        ))
    ]
    barrier = pltpu.get_barrier_semaphore()
    for d in range(1, n):
        pl.semaphore_signal(
            barrier, inc=1, device_id=(g, lax.rem(z + d, n)), device_id_type=MESH
        )
    for d in range(1, G):
        pl.semaphore_signal(
            barrier, inc=1, device_id=(lax.rem(g + d, G), z), device_id_type=MESH
        )
    for load in loads:
        load.start()
    ca[...] = jnp.zeros_like(ca)
    cb[...] = jnp.zeros_like(cb)
    loads[0].wait()
    loads[1].wait()
    def term(c, s):
        st = stages[s]
        lead = st.o % UNIT
        columns = pl.ds(pl.multiple_of(c * rows + (st.o - lead), UNIT), UNIT)
        whole = lax.dot_general(
            x[:, columns], ct[...], (((0,), (0,)), ((), ())), preferred_element_type=f32
        )
        return whole[lead : lead + st.R]

    def block(s):
        return pl.ds(stages[s].o, stages[s].R)

    def move(s, c, slot, to):
        return pltpu.make_async_remote_copy(
            src_ref=tb.at[c, block(s)], dst_ref=rb.at[slot, block(s)], send_sem=ts,
            recv_sem=tr.at[s, slot], device_id=(g, to), device_id_type=MESH,
        )

    def forward(s, k, ready=False):
        R = stages[s].R
        low = 2 * z < n
        nr = n - 1 - z
        right = jnp.where(low, jnp.where(k < nr, 1, 0), jnp.where(k < z, 0, 1)) == 1
        c = jnp.where(
            low, jnp.where(k < nr, n - 1 - k, k - nr), jnp.where(k < z, k, n - 1 - k + z)
        )
        to = jnp.where(right, z + 1, z - 1)
        slot = jnp.where(jnp.where(right, -1, z - 1) == c, n, c)
        if not ready:
            acc[pl.ds(0, R), :] = term(c, s)

            @pl.when(jnp.where(right, z, n - 1 - z) == 0)
            def _():
                tb[c, block(s), :] = acc[pl.ds(0, R), :].astype(bf16)

            @pl.when(jnp.where(right, z, n - 1 - z) > 0)
            def _():
                move(s, c, c, other_z).wait_recv()
                tb[c, block(s), :] = (acc[pl.ds(0, R), :] + rb[c, block(s), :].astype(f32)).astype(bf16)

        move(s, c, slot, to).start()

    def between(body):
        @pl.when((z > 0) & (z < n - 1))
        def _():
            body()

    def at_ends(body):
        @pl.when((z == 0) | (z == n - 1))
        def _():
            body()

    def place_of(s, p):
        st = stages[s]
        return (
            pl.ds(pl.multiple_of(st.o + p // st.nc * st.PR, TILE), st.PR),
            pl.ds(pl.multiple_of(lax.rem(p, st.nc) * st.PC, 128), st.PC),
        )

    def piece(s, p, to):
        st = stages[s]
        return pltpu.make_async_remote_copy(
            src_ref=pb.at[place_of(s, p)],
            dst_ref=rp.at[s, g, pl.ds(0, st.PR), pl.ds(0, st.PC)], send_sem=ps.at[s],
            recv_sem=pr.at[s], device_id=(to, z), device_id_type=MESH,
        )

    def pieces(s, k, sem):
        st = stages[s]
        several = rp.at[s, pl.ds(0, k), pl.ds(0, st.PR), pl.ds(0, st.PC)]
        return pltpu.make_async_copy(several, several, sem)

    def pieces_but_own(s, sem, count=None):
        st = stages[s]
        count = st.NP if count is None else count

        @pl.when(g < st.NP)
        def _():
            pieces(s, count - 1, sem).wait()

        if st.NP < G:
            @pl.when(g >= st.NP)
            def _():
                pieces(s, count, sem).wait()

    def inner(s):
        st = stages[s]
        R = st.R
        acc[pl.ds(0, R), :] = term(z, s)

        @pl.when(z > 0)
        def _():
            move(s, z, z, other_z).wait_recv()
            acc[pl.ds(0, R), :] += rb[z, block(s), :].astype(f32)

        @pl.when(z < n - 1)
        def _():
            move(s, z, n, other_z).wait_recv()
            acc[pl.ds(0, R), :] += rb[n, block(s), :].astype(f32)

        def tile(i, carry):
            at = pl.ds(pl.multiple_of(i * TILE, TILE), TILE)
            place = pl.ds(pl.multiple_of(st.o + i * TILE, TILE), TILE)
            first_row, second_row = fcol[place, :], scol[place, :]
            first_top, second_top = None, None
            for lane in lanes:
                gradient = acc[at, lane]
                codes = q[place, lane]
                first_code = (codes >> 4).astype(f32)
                second_code = (codes & 15).astype(f32) + 1.0
                first_new = (
                    jnp.minimum(first_row, fcm[:, lane]) * (first_code - 7.5)
                    + (1.0 - beta_one) * gradient
                )
                second_new = (
                    jnp.minimum(second_row, scm[:, lane]) * (second_code * second_code)
                    + (1.0 - beta_two) * gradient * gradient
                )
                fn[place, lane] = first_new
                sn[place, lane] = second_new
                update = (first_new * (inner_rate / bias_one)) / (
                    jnp.sqrt(second_new * (1.0 / bias_two)) + adam_eps
                )
                pseudo = update + (inner_rate * weight_decay) * w[place, lane].astype(f32)
                pb[place, lane] = pseudo.astype(bf16)
                size = jnp.abs(first_new)
                ca[:, lane] = jnp.maximum(ca[:, lane], size)
                cb[:, lane] = jnp.maximum(cb[:, lane], second_new)
                first_top = size if first_top is None else jnp.maximum(first_top, size)
                second_top = second_new if second_top is None else jnp.maximum(second_top, second_new)
            frn[place, :] = first_top
            srn[place, :] = second_top
            return carry

        lax.fori_loop(0, R // TILE, tile, 0)

        def send(d, carry):
            p = lax.rem(g + d, G)

            @pl.when(p < st.NP)
            def _():
                piece(s, p, p).start()

            return carry

        lax.fori_loop(1, G, send, 0)

    def plane_copy(s, c, p, to, sem):
        here = (av if c is None else wf.at[c]).at[place_of(s, p)]
        key = z if c is None else c
        return pltpu.make_async_remote_copy(
            src_ref=here, dst_ref=here, send_sem=hs.at[s],
            recv_sem=sem.at[s, key], device_id=(to, z), device_id_type=MESH,
        )

    def share(s, c):
        def send(d, carry):
            plane_copy(s, c, g, lax.rem(g + 2 * d, G), hr).start()
            return carry

        lax.fori_loop(1, G // 2, send, 0)
        plane_copy(s, c, g, mate, hm).start()

    def hand(s, c):
        st = stages[s]
        pieces_but_own(s, hr.at[s, z if c is None else c], st.NP // 2)

        def send(d, carry):
            p = lax.rem(g + 2 * d, G)

            @pl.when(p < st.NP)
            def _():
                plane_copy(s, c, p, mate, hm).start()

            return carry

        lax.fori_loop(1, G // 2, send, 0)

    def arrived(s, c):
        pieces(s, stages[s].NP // 2, hm.at[s, z if c is None else c]).wait()

    def reduce(s):
        st = stages[s]
        top = (pl.ds(0, st.PR), pl.ds(0, st.PC))

        @pl.when(g < st.NP)
        def _():
            pieces(s, G - 1, pr.at[s]).wait()
            acc[top] = pb[place_of(s, g)].astype(f32)

            def add(d, carry):
                acc[top] += rp[(s, lax.rem(g + d, G)) + top].astype(f32)
                return carry

            lax.fori_loop(1, G, add, 0)
            averaged = (acc[top] * (1.0 / G)).astype(bf16)
            av[place_of(s, g)] = averaged
            averaged = averaged.astype(f32)
            momentum = outer_beta * m[place_of(s, g)] + averaged
            fresh = w[place_of(s, g)].astype(f32) - outer_rate * (averaged + outer_beta * momentum)
            wo[(s,) + top] = fresh.astype(bf16)

            if s < NEAR:
                between(lambda: to_planes(s))

                @pl.when(z == 0)
                def _():
                    own_piece(s, z + 1).start()

                @pl.when(z == n - 1)
                def _():
                    own_piece(s, z - 1).start()
            elif s == held:
                pass
            else:
                to_planes(s)

            share(s, None)

    def own_piece(s, to):
        st = stages[s]
        return pltpu.make_async_remote_copy(
            src_ref=wo.at[s, pl.ds(0, st.PR), pl.ds(0, st.PC)],
            dst_ref=wf.at[(z,) + place_of(s, g)], send_sem=zs.at[s],
            recv_sem=gr.at[s, z], device_id=(g, to), device_id_type=MESH,
        )

    def to_planes(s):
        for d in range(1, n):
            own_piece(s, lax.rem(z + d, n)).start()

    def passed(s, c, to):
        here = wf.at[(c,) + place_of(s, g)]
        return pltpu.make_async_remote_copy(
            src_ref=here, dst_ref=here, send_sem=zf.at[s],
            recv_sem=gr.at[s, c], device_id=(g, to), device_id_type=MESH,
        )

    def spread(s, c):
        @pl.when(g < stages[s].NP)
        def _():
            passed(s, c, other_z).wait_recv()
            if s < NEAR:
                @pl.when((c == 0) & (z == 1))
                def _():
                    for to in range(2, n):
                        passed(s, c, to).start()

                @pl.when((c == n - 1) & (z == n - 2))
                def _():
                    for to in range(n - 2):
                        passed(s, c, to).start()

            share(s, c)

    def over_mid(body, s):
        def step(c, carry):
            @pl.when(c != z)
            def _():
                body(s, c)

            return carry

        lax.fori_loop(1, n - 1, step, 0)

    def over_near(body, s):
        if n > 2:
            @pl.when(z == 1)
            def _():
                body(s, 0)

            @pl.when(z == n - 2)
            def _():
                body(s, n - 1)

    def over_far(body, s):
        @pl.when((z != 0) & ((z != 1) | (n == 2)))
        def _():
            body(s, 0)

        @pl.when((z != n - 1) & ((z != n - 2) | (n == 2)))
        def _():
            body(s, n - 1)

    def outer(s):
        st = stages[s]
        arrived(s, None)

        def tile(i, carry):
            place = pl.ds(pl.multiple_of(st.o + i * TILE, TILE), TILE)
            averaged = av[place, :].astype(f32)
            momentum = outer_beta * m[place, :] + averaged
            fresh = w[place, :].astype(f32) - outer_rate * (averaged + outer_beta * momentum)
            o_m[place, :] = momentum
            o_w[place, :] = fresh
            wf[z, place, :] = fresh.astype(bf16)
            return carry

        lax.fori_loop(0, st.R // TILE, tile, 0)
    def turn(s, k):
        at = s + k / max(1, n - 2)
        return at - 0.99 if s == S - 1 and k < n - 2 else at

    order = sorted((turn(s, k), k, s) for s in range(S) for k in range(n - 1))

    def send_group(first, last):
        @at_ends
        def _():
            for at, k, s in order:
                if first <= at < last:
                    forward(s, k, ready=(s, k) == (0, 0))

    done = set()

    def once(name, body, *key):
        if min(key[:1]) >= 0 and (name, key) not in done:
            done.add((name, key))
            with jax.named_scope(f"{name}{'_'.join(str(k) for k in key if isinstance(k, int))}"):
                body()

    def do(over, body, t):
        once(body.__name__ + over.__name__[4:], lambda: over(body, t), t)

    far = jnp.where(2 * z < n, n - 1, 0)

    @at_ends
    def _():
        tb[far, block(0), :] = term(far, 0).astype(bf16)

    with jax.named_scope("barrier"):
        pl.semaphore_wait(barrier, G - 1 + n - 1)
    paced = S > 3
    send_group(0, 2 if paced else S + 1)

    for load in loads[2:]:
        load.wait()
    fcm[...] = fcm[...] * (beta_one / 7.5)
    scm[...] = scm[...] * (beta_two / 256.0)
    for o in range(0, rows, UNIT):
        part = pl.ds(o, UNIT)
        fcol[part, :] = to_column(frm[:, part] * (beta_one / 7.5))
        scol[part, :] = to_column(srm[:, part] * (beta_two / 256.0))

    def column_max(slot, to):
        return pltpu.make_async_remote_copy(
            src_ref=cmb.at[z], dst_ref=cmb.at[z], send_sem=cs,
            recv_sem=cr, device_id=(g, to), device_id_type=MESH,
        )

    def all_column_max(sem):
        several = cmb.at[pl.ds(0, n - 1)]
        return pltpu.make_async_copy(several, several, sem)

    def forward_rest(s):
        def step(k, carry):
            forward(s, k)
            return carry

        lax.fori_loop(1, n - 1, step, 0)

    def row_max(s):
        part = block(s)
        first = jnp.max(frn[part, :], axis=1, keepdims=True) + stat_eps
        second = jnp.max(srn[part, :], axis=1, keepdims=True) + stat_eps
        frn[part, :] = jnp.broadcast_to(first, (stages[s].R, 128))
        srn[part, :] = jnp.broadcast_to(second, (stages[s].R, 128))

    def rows_out():
        for o in range(0, rows, UNIT):
            part = pl.ds(o, UNIT)
            o_frm[:, part] = frn[part, :].T[:1, :]
            o_srm[:, part] = srn[part, :].T[:1, :]

    def far_chunk(s):
        once("fwA", lambda: between(functools.partial(forward, s, 0)), s)

    def near_chunks(s):
        once("fwB", lambda: between(functools.partial(forward_rest, s)), s)

    for s in range(S - 1):
        far_chunk(s)
        if s == S - 2 and s - 2 < NEAR:
            do(over_near, spread, s - 2)
        if s >= 1:
            once("inner", lambda: inner(s - 1), s - 1)
        if s == S - 2:
            far_chunk(s + 1)
        do(over_mid, spread, s - 2)
        if s - 2 < NEAR:
            do(over_near, spread, s - 2)
        if s - 3 < NEAR:
            do(over_far, spread, s - 3)
        once("handav", lambda: hand(s - 2, None), s - 2)
        do(over_mid, hand, s - 3)
        if s - 3 < NEAR:
            do(over_near, hand, s - 3)
        if s - 4 < NEAR:
            do(over_far, hand, s - 4)
        if s >= 1:
            row_max(s - 1)
        near_chunks(s)
        once("reduce", lambda: reduce(s - 1), s - 1)
        if s == S - 2:
            near_chunks(s + 1)
            if held >= NEAR:
                @between
                def _():
                    @pl.when(g < stages[held].NP)
                    def _():
                        to_planes(held)
            once("outer", lambda: outer(s - 2), s - 2)
        if s < S - 2:
            once("outer", lambda: outer(s - 2), s - 2)
        if paced and s in (1, 2):
            with jax.named_scope(f"group{s+1}"):
                send_group(s + 1, s + 2 if s == 1 else S + 1)
    once("inner", lambda: inner(S - 2), S - 2)
    if S - 4 < NEAR:
        do(over_far, spread, S - 4)
    once("handav", lambda: hand(S - 3, None), S - 3)

    def last_inner():
        if held >= NEAR:
            @at_ends
            def _():
                chunks = tb.at[pl.ds(0, n - 1)]
                pltpu.make_async_copy(chunks, chunks, ts).wait()

                @pl.when(g < stages[held].NP)
                def _():
                    to_planes(held)

        inner(S - 1)
        cmb[z, pl.ds(0, 1), :] = jnp.max(ca[...], axis=0, keepdims=True)
        cmb[z, pl.ds(1, 1), :] = jnp.max(cb[...], axis=0, keepdims=True)
        for d in range(1, n):
            column_max(d, lax.rem(z + d, n)).start()

    def states():
        all_column_max(cr).wait()
        scales = jnp.max(cmb[...], axis=0) + stat_eps
        o_fcm[...] = scales[0:1]
        o_scm[...] = scales[1:2]
        fcm[...] = 1.0 / o_fcm[...]
        scm[...] = 1.0 / o_scm[...]

        def tile(i, carry):
            place = pl.ds(pl.multiple_of(i * TILE, TILE), TILE)
            first_row, second_row = 1.0 / frn[place, :], 1.0 / srn[place, :]
            for lane in lanes:
                o_fs[place, lane] = (fn[place, lane] * jnp.maximum(first_row, fcm[:, lane])).astype(bf16)
                o_ss[place, lane] = (sn[place, lane] * jnp.maximum(second_row, scm[:, lane])).astype(bf16)
            return carry

        lax.fori_loop(0, rows // TILE, tile, 0)

    def product(c, o, width):
        columns = pl.ds(pl.multiple_of(c * rows + o, UNIT), width)
        return jnp.dot(x[:, columns], wf[c, pl.ds(o, width), :], preferred_element_type=f32)

    def others(body):
        def step(j, carry):
            for c in (z - j, z + j):
                @pl.when((c >= 0) & (c < n))
                def _():
                    body(c)

            return carry

        lax.fori_loop(1, n, step, 0)

    def gather_early(c):
        for s in range(S - 2):
            arrived(s, c)
        keys[...] += product(c, 0, cut)

    def gather_mid(c):
        @pl.when((c > 0) & (c < n - 1))
        def _():
            gather_early(c)

    def gather_end(c):
        @pl.when((c == 0) | (c == n - 1))
        def _():
            gather_early(c)

    def own():
        if cut:
            keys[...] = product(z, 0, cut)
        else:
            keys[...] = jnp.zeros_like(keys)

    def run(name, body):
        with jax.named_scope(name):
            body()

    everywhere = (over_mid, over_near, over_far)
    run("lastinner", last_inner)
    for t in range(S - 2):
        for over in everywhere:
            do(over, spread, t)
    once("reduce", lambda: reduce(S - 2), S - 2)
    row_max(S - 2)
    row_max(S - 1)
    run("rowsout", rows_out)
    for t in range(S - 2):
        once("handav", functools.partial(hand, t, None), t)
        once("outer", functools.partial(outer, t), t)
    once("reduce", lambda: reduce(S - 1), S - 1)
    for over in everywhere:
        do(over, spread, S - 2)
    once("handav", lambda: hand(S - 2, None), S - 2)
    run("states", states)
    run("own", own)
    for t in range(S - 2):
        for over in everywhere:
            do(over, hand, t)
    for over in everywhere:
        do(over, spread, S - 1)
    once("handav", lambda: hand(S - 1, None), S - 1)
    once("outer", lambda: outer(S - 2), S - 2)
    for over in everywhere:
        do(over, hand, S - 2)
    if cut:
        run("gmid", functools.partial(others, gather_mid))
        run("gend", functools.partial(others, gather_end))
    for over in everywhere:
        do(over, hand, S - 1)
    once("outer", lambda: outer(S - 1), S - 1)

    def last_pieces(c):
        for s in (S - 2, S - 1):
            arrived(s, c)

    run("lastpieces", functools.partial(others, last_pieces))

    def last_product():
        TT = UNIT

        def tile(i, carry):
            tokens = pl.ds(pl.multiple_of(i * TT, TT), TT)
            total = keys[tokens, :]
            for c in range(0, n, 2):
                pair = range(c, min(n, c + 2))
                left = [x[tokens, pl.ds(k * rows + cut, UNIT)] for k in pair]
                right = [wf[k, pl.ds(cut, UNIT), :] for k in pair]
                total += jnp.dot(
                    jnp.concatenate(left, axis=1), jnp.concatenate(right, axis=0),
                    preferred_element_type=f32,
                )
            o_k[tokens, :] = total.astype(bf16)
            return carry

        lax.fori_loop(0, x.shape[0] // TT, tile, 0)

    run("lastprod", last_product)

    def sends():
        def pieces_sent():
            chunks = tb.at[pl.ds(0, n - 1)]
            pltpu.make_async_copy(chunks, chunks, ts).wait()

        if held >= NEAR:
            between(pieces_sent)
        else:
            pieces_sent()

        for s in range(S):
            pieces_but_own(s, ps.at[s])

        def spread_sent(s, k):
            st = stages[s]
            several = rp.at[pl.ds(0, n), pl.ds(0, k), pl.ds(0, st.PR), pl.ds(0, st.PC)]
            pltpu.make_async_copy(several, several, hs.at[s]).wait()

        for s in range(S):
            half = stages[s].NP // 2

            @pl.when(g < stages[s].NP)
            def _():
                spread_sent(s, G // 2 + half - 1)

            if stages[s].NP < G:
                @pl.when(g >= stages[s].NP)
                def _():
                    spread_sent(s, half)

        for s in range(S):
            @pl.when(g < stages[s].NP)
            def _():
                if s >= NEAR:
                    pieces(s, n - 1, zs.at[s]).wait()
                else:
                    between(lambda: pieces(s, n - 1, zs.at[s]).wait())
                    at_ends(lambda: pieces(s, 1, zs.at[s]).wait())
                    if n > 3:
                        @pl.when((z == 1) | (z == n - 2))
                        def _():
                            pieces(s, n - 2, zf.at[s]).wait()

        all_column_max(cs).wait()

    run("sends", sends)


def finish(*refs):
    k = (len(refs) - 1) // 2
    sems = refs[-1]
    copies = [
        pltpu.make_async_copy(src, dst, sems.at[i])
        for i, (src, dst) in enumerate(zip(refs[:k], refs[k:-1]))
    ]
    for copy in copies:
        copy.start()
    for copy in copies:
        copy.wait()


def local(x, ct, w, m, q, frm, fcm, srm, scm):
    n, G = lax.axis_size("fsdp"), lax.axis_size("grp")
    rows, C = w.shape
    T, K = x.shape[1:]
    stages = plan(rows, C, G)
    S = len(stages)
    PR = max(st.PR for st in stages)
    hbm = pl.BlockSpec(memory_space=pltpu.HBM)
    vmem = pl.BlockSpec(memory_space=pltpu.VMEM)
    dma = pltpu.SemaphoreType.DMA
    shape = jax.ShapeDtypeStruct
    outs = pl.pallas_call(
        functools.partial(kernel, n, G, stages),
        out_shape=(
            pltpu.VMEM((rows, C), f32), pltpu.VMEM((rows, C), f32),
            pltpu.VMEM((rows, C), bf16), pltpu.VMEM((rows, C), bf16),
            pltpu.VMEM((1, rows), f32), pltpu.VMEM((1, C), f32),
            pltpu.VMEM((1, rows), f32), pltpu.VMEM((1, C), f32),
            pltpu.VMEM((T, C), bf16),
        ),
        in_specs=[hbm] * 9,
        out_specs=(vmem,) * 9,
        scratch_shapes=[
            pltpu.VMEM((T, K), bf16), pltpu.VMEM((T, C), bf16), pltpu.VMEM((rows, C), bf16),
            pltpu.VMEM((rows, C), f32), pltpu.VMEM((rows, C), jnp.int32),
            pltpu.VMEM((1, rows), f32), pltpu.VMEM((1, C), f32),
            pltpu.VMEM((1, rows), f32), pltpu.VMEM((1, C), f32),
            pltpu.VMEM((n, rows, C), bf16), pltpu.VMEM((n + 1, rows, C), bf16),
            pltpu.VMEM((rows, C), bf16), pltpu.VMEM((max(S, n), G, PR, C), bf16),
            pltpu.VMEM((rows, C), bf16), pltpu.VMEM((S, PR, C), bf16), pltpu.VMEM((n, rows, C), bf16),
            pltpu.VMEM((rows, C), f32), pltpu.VMEM((rows, C), f32),
            pltpu.VMEM((UNIT, C), f32), pltpu.VMEM((T, C), f32),
            pltpu.VMEM((rows, 128), f32), pltpu.VMEM((rows, 128), f32),
            pltpu.VMEM((rows, 128), f32), pltpu.VMEM((rows, 128), f32),
            pltpu.VMEM((TILE, C), f32), pltpu.VMEM((TILE, C), f32), pltpu.VMEM((n, 2, C), f32),
            dma((9,)), dma, dma((S, n + 1)), dma((S,)), dma((S,)), dma((S,)), dma((S,)),
            dma((S, n)), dma((S,)), dma((S, n)), dma((S, n)), dma, dma,
        ],
        compiler_params=pltpu.CompilerParams(
            collective_id=0, has_side_effects=True, vmem_limit_bytes=54 * 1024 * 1024
        ),
    )(x[0], ct[0], w, m, q[0], frm, fcm, srm, scm)
    done = pl.pallas_call(
        finish,
        out_shape=tuple(shape(a.shape, a.dtype) for a in outs),
        in_specs=(vmem,) * 9,
        out_specs=(hbm,) * 9,
        scratch_shapes=[dma((9,))],
        compiler_params=pltpu.CompilerParams(vmem_limit_bytes=8 * 1024 * 1024),
    )(*outs)
    new_w, new_m, fs, ss, nfr, nfc, nsr, nsc, keys = done
    return new_w, new_m, fs[None], ss[None], nfr, nfc, nsr, nsc, keys[None]


def solution(mesh):
    return jax.shard_map(
        local,
        mesh=mesh,
        in_specs=(
            P("grp", "fsdp", None), P("grp", "fsdp", None), P("fsdp", None), P("fsdp", None),
            P("grp", "fsdp", None), P("grp", "fsdp"), P("grp", None), P("grp", "fsdp"),
            P("grp", None),
        ),
        out_specs=(
            P("fsdp", None), P("fsdp", None), P("grp", "fsdp", None), P("grp", "fsdp", None),
            P("grp", "fsdp"), P("grp", None), P("grp", "fsdp"), P("grp", None),
            P("grp", "fsdp", None),
        ),
        check_vma=False,
    )
```
